32 devices in a mesh: row: 4 (over y, core), col: 8 (over z, x).
Axes of the slice: x: 2, y: 2, z: 4, core: 2. Of those that a mesh axis runs over, the one named last changes fastest.
Arguments:
- velocity_modes: bfloat16 [3, 176, 352, 704], P(None, 'row', 'col'), may hold values from -0.00090789795 to 0.00090789795
- wavenumbers: float32 [8], replicated, may hold values from 0.5 to 3
- polar: float32 [8], replicated, may hold values from -3.140625 to 3.140625
- azimuth: float32 [8], replicated, may hold values from -3.140625 to 3.140625
Outputs:
- velocity: bfloat16 [3, 512, 512, 512], P(None, 'row', 'col')
- far_field: float32 [8, 2, 8], P('col')
The draws below stay inside these ranges and needn't reach their ends.
All inputs are finite; a program needn't handle non-finite values.
Results may differ from the reference program's by a relative error of at most 0.0075.
Values may be sent and summed in bfloat16 or wider, within the bound.
A program may use at most 192 MiB of HBM per device.

```python
import math
import jax
import jax.numpy as jnp
from jax import lax

N = 512
M = 352
KX = 176
FREQS = 8
DIRS = 8


def levels(rng, extent, split, low, largest):
    factor_of, own = 1.0, jax.random.fold_in(rng, 6)
    for axis_at, blocks in split:
        draws = jnp.exp(jax.random.uniform(jax.random.fold_in(own, axis_at), (blocks,), jnp.float32, low / len(split), largest / len(split)))
        factor_of = factor_of * jnp.repeat(draws, extent[axis_at] // blocks).reshape([-1 if axis == axis_at else 1 for axis in range(len(extent))])
    return factor_of


def scatter_about(key, shape, width, most, cuts=(), kind=jnp.bfloat16):
    factor_of = levels(key, shape, cuts, -0.22, 0.18) if cuts else 1.0
    drawn = jax.random.normal(key, shape, jnp.float32) * width * factor_of
    return jnp.minimum(jnp.maximum(drawn, -most), most).astype(kind)


def setup_inputs(seed: int = 0) -> dict:
    streams_of = jax.random.split(jax.random.key(seed), 5)
    return {
        "velocity_modes": scatter_about(streams_of[0], (3, KX, M, 2 * M), (M ** -1.5), 0.00090789795, ((1, 4), (2, 8))),
        "wavenumbers": jnp.clip(jnp.exp(jax.random.uniform(streams_of[1], (FREQS,), jnp.float32, math.log(0.5), math.log(3.0))), 0.5, 3.0),
        "polar": jnp.clip(jax.random.uniform(streams_of[2], (DIRS,), jnp.float32, -3.140625, 3.140625), -3.140625, 3.140625),
        "azimuth": jnp.clip(jax.random.uniform(streams_of[3], (DIRS,), jnp.float32, -3.140625, 3.140625), -3.140625, 3.140625),
    }


def complex_table(modes, points):
    waves = jnp.arange(modes, dtype=jnp.int32) - modes // 2
    cells = jnp.arange(points, dtype=jnp.int32)
    product = jnp.mod(waves[:, None] * cells[None, :], points)
    angle = product.astype(jnp.float32) * (2.0 * math.pi / points)
    cosine = jnp.cos(angle)
    sine = jnp.sin(angle)
    table = jnp.stack([jnp.stack([cosine, sine], 1), jnp.stack([-sine, cosine], 1)], 0)
    return table.astype(jnp.bfloat16)


def half_table(count, points):
    waves = jnp.arange(count, dtype=jnp.int32)
    cells = jnp.arange(points, dtype=jnp.int32)
    product = jnp.mod(waves[:, None] * cells[None, :], points)
    angle = product.astype(jnp.float32) * (2.0 * math.pi / points)
    cosine = jnp.cos(angle).astype(jnp.bfloat16)
    sine = jnp.sin(angle).astype(jnp.bfloat16)
    factor = jnp.where(waves == 0, 1.0, 2.0).astype(jnp.bfloat16)[:, None]
    return jnp.stack([factor * cosine, -(factor * sine)], 0)


def stresses(field):
    trace = (field[0] * field[0] + field[1] * field[1] + field[2] * field[2]) / 3.0
    parts = [field[0] * field[0] - trace, field[1] * field[1] - trace, field[2] * field[2] - trace,
             field[0] * field[1], field[0] * field[2], field[1] * field[2]]
    return jnp.stack(parts, 0).astype(jnp.bfloat16)


def far_terms(stress, wave_j, axis_one, axis_two, axis_three, y_pos, z_pos):
    points = stress.shape[-1]
    y_count = stress.shape[1]
    z_count = stress.shape[2]
    count = wave_j.shape[0]
    x_pos = jnp.arange(points, dtype=jnp.int32).astype(jnp.float32) * (2.0 * math.pi / points)
    angle_x = wave_j[None, :] * (axis_one[None, :] * x_pos[:, None])
    phase_x = jnp.stack([jnp.cos(angle_x), -jnp.sin(angle_x)], 1).reshape(points, 2 * count).astype(jnp.bfloat16)
    lines = jnp.dot(stress.reshape(6 * y_count * z_count, points), phase_x, preferred_element_type=jnp.float32)
    lines = lines.reshape(6, y_count, z_count, 2, count)
    weights = [axis_one * axis_one, axis_two * axis_two, axis_three * axis_three,
               2.0 * axis_one * axis_two, 2.0 * axis_one * axis_three, 2.0 * axis_two * axis_three]
    mixed = weights[0][None, None, None, :] * lines[0]
    for index in range(1, 6):
        mixed = mixed + weights[index][None, None, None, :] * lines[index]
    angle = wave_j[None, None, :] * (axis_two[None, None, :] * y_pos[:, None, None]) + wave_j[None, None, :] * (axis_three[None, None, :] * z_pos[None, :, None])
    cosine = jnp.cos(angle)
    sine = jnp.sin(angle)
    real_part = mixed[:, :, 0, :]
    imag_part = mixed[:, :, 1, :]
    return jnp.stack([jnp.sum(real_part * cosine + imag_part * sine, (0, 1)),
                      jnp.sum(imag_part * cosine - real_part * sine, (0, 1))], 0)


def reference(velocity_modes, wavenumbers, polar, azimuth):
    table = complex_table(M, N)
    table_x = half_table(KX, N)
    modes = velocity_modes.reshape(3, KX, M, 2, M)

    def along_z(component):
        return jnp.einsum("abpk,pkqz->azqb", component.astype(jnp.float32), table.astype(jnp.float32)).astype(jnp.bfloat16)

    first = lax.map(along_z, modes)

    def along_y(component):
        return jnp.einsum("azpb,pbqy->yzqa", component.astype(jnp.float32), table.astype(jnp.float32)).astype(jnp.bfloat16)

    second = lax.map(along_y, first)
    dirs = polar.shape[0]
    wave_j = jnp.repeat(wavenumbers, dirs)
    axis_one = jnp.tile(jnp.sin(polar) * jnp.cos(azimuth), FREQS)
    axis_two = jnp.tile(jnp.sin(polar) * jnp.sin(azimuth), FREQS)
    axis_three = jnp.tile(jnp.cos(polar), FREQS)
    block = 8
    z_pos = jnp.arange(N, dtype=jnp.int32).astype(jnp.float32) * (2.0 * math.pi / N)

    def one_block(number):
        start = (number * block).astype(jnp.int32)
        piece = lax.dynamic_slice_in_dim(second, start, block, 1)
        field = jnp.einsum("cyzpa,pax->cyzx", piece.astype(jnp.float32), table_x.astype(jnp.float32))
        stress = stresses(field)
        y_pos = (start + jnp.arange(block, dtype=jnp.int32)).astype(jnp.float32) * (2.0 * math.pi / N)
        terms = far_terms(stress, wave_j, axis_one, axis_two, axis_three, y_pos, z_pos)
        return field.astype(jnp.bfloat16), terms

    blocks, terms = lax.map(one_block, jnp.arange(N // block, dtype=jnp.int32))
    velocity = jnp.transpose(blocks, (1, 0, 2, 3, 4)).reshape(3, N, N, N)
    spectrum = jnp.sum(terms, 0).reshape(2, FREQS, dirs)
    spectrum = spectrum * (wavenumbers * wavenumbers)[None, :, None] / (N ** 1.5)
    far_field = jnp.transpose(spectrum, (2, 0, 1))
    return velocity, far_field
```

```python
import functools
import math

import jax
import jax.numpy as jnp
from jax import lax
from jax.experimental import pallas as pl
from jax.experimental.pallas import tpu as pltpu
from jax.sharding import PartitionSpec as P

VMEM_LIMIT = 60 * 1024 * 1024


def padded(count):
    return -(-count // 16) * 16


def angles(waves, points):
    cells = jnp.arange(points, dtype=jnp.int32)
    product = jnp.mod(waves[:, None] * cells[None, :], points)
    return product.astype(jnp.float32) * (2.0 * math.pi / points)


def z_table(modes, points, blocks):
    angle = angles(jnp.arange(modes, dtype=jnp.int32) - modes // 2, points)
    cosine = jnp.cos(angle).reshape(modes, blocks, 1, -1)
    sine = jnp.sin(angle).reshape(modes, blocks, 1, -1)
    table = jnp.concatenate(
        [jnp.concatenate([cosine, sine], 2), jnp.concatenate([-sine, cosine], 2)], 0
    )
    return table.reshape(2 * modes, 2 * points).astype(jnp.bfloat16)


def y_table(modes, points, sources, blocks):
    angle = angles(jnp.arange(modes, dtype=jnp.int32) - modes // 2, points).T
    both = jnp.stack([jnp.cos(angle), jnp.sin(angle)], 0)
    both = both.reshape(2, blocks, points // blocks, sources, modes // sources)
    extra = padded(modes // sources) - modes // sources
    both = jnp.pad(both, ((0, 0), (0, 0), (0, 0), (0, 0), (0, extra)))
    both = jnp.transpose(both, (1, 0, 2, 3, 4))
    return both.reshape(blocks, 2 * (points // blocks), -1).astype(jnp.bfloat16)


def x_table(count, points, sources):
    waves = jnp.arange(count, dtype=jnp.int32)
    angle = angles(waves, points)
    cosine = jnp.cos(angle).astype(jnp.bfloat16)
    sine = jnp.sin(angle).astype(jnp.bfloat16)
    factor = jnp.where(waves == 0, 1.0, 2.0).astype(jnp.bfloat16)[:, None]
    table = jnp.stack([factor * cosine, -(factor * sine)], 0)
    table = table.reshape(2, sources, count // sources, points)
    extra = padded(count // sources) - count // sources
    table = jnp.pad(table, ((0, 0), (0, 0), (0, extra), (0, 0)))
    return table.reshape(2, -1, points)


def estimate(rows, depth, columns):
    return pl.CostEstimate(
        flops=2 * rows * depth * columns,
        bytes_accessed=2 * (rows * depth + depth * columns + rows * columns),
        transcendentals=0,
    )


def along_z(modes_ref, table_ref, out_ref):
    slabs, ky = modes_ref.shape[1], modes_ref.shape[2]
    blocks, width = out_ref.shape[0], out_ref.shape[4]

    @pl.loop(0, slabs)
    def _(a):
        value = jnp.dot(modes_ref[0, a], table_ref[...], preferred_element_type=jnp.float32)
        value = value.astype(jnp.bfloat16)
        for block in range(blocks):
            out_ref[block, 0, a] = jnp.zeros(out_ref.shape[3:], jnp.bfloat16)
            out_ref[block, 0, a, 0:ky, :] = value[:, block * width : (block + 1) * width]


def along_y(moved_ref, table_ref, out_ref, total):
    slabs, width = moved_ref.shape[2], moved_ref.shape[4]
    half = width // 2
    rows = out_ref.shape[2]
    total[...] = jnp.zeros_like(total)
    group = 2 if slabs % 2 == 0 and width % 128 == 0 else 1
    for a in range(0, slabs, group):
        parts = [moved_ref[:, 0, a + g].reshape(-1, width) for g in range(group)]
        data = parts[0] if group == 1 else jnp.concatenate(parts, 1)
        product = jnp.dot(table_ref[0], data, preferred_element_type=jnp.float32)
        for g in range(group):
            by_cos = product[:rows, g * width : (g + 1) * width]
            by_sin = product[rows:, g * width : (g + 1) * width]
            turned = jnp.concatenate([-by_sin[:, half:], by_sin[:, :half]], 1)
            total[:, a + g, :] = by_cos + turned
    out_ref[0, 0] = total[...].astype(jnp.bfloat16)


def along_x(arrived_0, arrived_1, arrived_2, table_ref, phase_ref, weight_ref, cos_ref, sin_ref,
            velocity_ref, by_cos_ref, by_sin_ref, real_scr, imag_scr):
    ys, width = arrived_0.shape[2], arrived_0.shape[4]
    half = width // 2
    fields = []
    for c, arrived_ref in enumerate((arrived_0, arrived_1, arrived_2)):
        for y in range(ys):
            data = arrived_ref[:, 0, y].reshape(-1, width).T
            real_scr[c, y * half : (y + 1) * half, :] = data[:half]
            imag_scr[c, y * half : (y + 1) * half, :] = data[half:]
        field = jnp.dot(real_scr[c], table_ref[0], preferred_element_type=jnp.float32)
        field = field + jnp.dot(imag_scr[c], table_ref[1], preferred_element_type=jnp.float32)
        velocity_ref[c] = field.astype(jnp.bfloat16).reshape(velocity_ref.shape[1:])
        fields.append(field)
    f0, f1, f2 = fields
    trace = (f0 * f0 + f1 * f1 + f2 * f2) / 3.0
    stress = [f0 * f0 - trace, f1 * f1 - trace, f2 * f2 - trace, f0 * f1, f0 * f2, f1 * f2]
    mixed = None
    for index, part in enumerate(stress):
        line = jnp.dot(
            part.astype(jnp.bfloat16), phase_ref[...], preferred_element_type=jnp.float32
        )
        term = weight_ref[index : index + 1, :] * line
        mixed = term if mixed is None else mixed + term
    mixed = mixed.reshape(ys, half, -1)
    by_cos_ref[...] = jnp.sum(mixed * cos_ref[...][None], 1)
    by_sin_ref[...] = jnp.sum(mixed * sin_ref[...][None], 1)


def body(rows, cols, velocity_modes, wavenumbers, polar, azimuth):
    kx_local, ky_local, modes = velocity_modes.shape[1:]
    modes = modes // 2
    kx = kx_local * rows
    points = velocity_points(modes)
    y_local, z_local = points // rows, points // cols
    width = 2 * z_local
    ky_pad, kx_pad = padded(ky_local), padded(kx_local)

    table_z = z_table(modes, points, cols)
    table_y = y_table(modes, points, cols, rows)
    steps = 2 if kx_local % 2 == 0 else 1
    slabs = kx_local // steps
    arrived = []
    for c in range(3):
        first = pl.pallas_call(
            along_z,
            grid=(steps,),
            in_specs=[
                pl.BlockSpec((1, slabs, ky_local, 2 * modes), lambda i, c=c: (c, i, 0, 0)),
                pl.BlockSpec((2 * modes, 2 * points), lambda i: (0, 0)),
            ],
            out_specs=pl.BlockSpec((cols, 1, slabs, ky_pad, width), lambda i: (0, 0, i, 0, 0)),
            out_shape=jax.ShapeDtypeStruct((cols, 1, kx_local, ky_pad, width), jnp.bfloat16),
            compiler_params=pltpu.CompilerParams(vmem_limit_bytes=VMEM_LIMIT),
            cost_estimate=estimate(kx_local * ky_pad, 2 * modes, 2 * points),
            name=f"along_z_{c}",
        )(velocity_modes, table_z)
        moved = lax.all_to_all(first, "col", split_axis=0, concat_axis=0, tiled=True)
        second = pl.pallas_call(
            along_y,
            grid=(rows,),
            in_specs=[
                pl.BlockSpec((cols, 1, kx_local, ky_pad, width), lambda t: (0, 0, 0, 0, 0)),
                pl.BlockSpec((1, 2 * y_local, cols * ky_pad), lambda t: (t, 0, 0)),
            ],
            out_specs=pl.BlockSpec((1, 1, y_local, kx_pad, width), lambda t: (t, 0, 0, 0, 0)),
            out_shape=jax.ShapeDtypeStruct((rows, 1, y_local, kx_pad, width), jnp.bfloat16),
            scratch_shapes=[pltpu.VMEM((y_local, kx_pad, width), jnp.float32)],
            compiler_params=pltpu.CompilerParams(vmem_limit_bytes=VMEM_LIMIT),
            cost_estimate=estimate(2 * points, cols * ky_pad, kx_local * width),
            name=f"along_y_{c}",
        )(moved, table_y)
        arrived.append(lax.all_to_all(second, "row", split_axis=0, concat_axis=0, tiled=True))

    dirs, freqs = polar.shape[0], wavenumbers.shape[0]
    count = dirs * freqs
    wave_j = jnp.repeat(wavenumbers, dirs)
    axis_one = jnp.tile(jnp.sin(polar) * jnp.cos(azimuth), freqs)
    axis_two = jnp.tile(jnp.sin(polar) * jnp.sin(azimuth), freqs)
    axis_three = jnp.tile(jnp.cos(polar), freqs)
    unit = 2.0 * math.pi / points
    x_pos = jnp.arange(points, dtype=jnp.int32).astype(jnp.float32) * unit
    angle_x = wave_j[None, :] * (axis_one[None, :] * x_pos[:, None])
    phase_x = jnp.concatenate([jnp.cos(angle_x), -jnp.sin(angle_x)], 1).astype(jnp.bfloat16)
    weights = jnp.stack(
        [
            axis_one * axis_one,
            axis_two * axis_two,
            axis_three * axis_three,
            2.0 * axis_one * axis_two,
            2.0 * axis_one * axis_three,
            2.0 * axis_two * axis_three,
        ],
        0,
    )
    weights = jnp.concatenate([weights, weights], 1)
    z_index = lax.axis_index("col") * z_local + jnp.arange(z_local, dtype=jnp.int32)
    y_index = lax.axis_index("row") * y_local + jnp.arange(y_local, dtype=jnp.int32)
    angle_z = wave_j[None, :] * (axis_three[None, :] * (z_index.astype(jnp.float32) * unit)[:, None])
    angle_y = wave_j[None, :] * (axis_two[None, :] * (y_index.astype(jnp.float32) * unit)[:, None])
    cos_z, sin_z = jnp.cos(angle_z), jnp.sin(angle_z)

    ys = 8
    whole = lambda i: (0, 0)
    velocity, by_cos, by_sin = pl.pallas_call(
        along_x,
        grid=(y_local // ys,),
        in_specs=[
            *[pl.BlockSpec((rows, 1, ys, kx_pad, width), lambda i: (0, 0, i, 0, 0))] * 3,
            pl.BlockSpec((2, rows * kx_pad, points), lambda i: (0, 0, 0)),
            pl.BlockSpec((points, 2 * count), whole),
            pl.BlockSpec((6, 2 * count), whole),
            pl.BlockSpec((z_local, 2 * count), whole),
            pl.BlockSpec((z_local, 2 * count), whole),
        ],
        out_specs=[
            pl.BlockSpec((3, ys, z_local, points), lambda i: (0, i, 0, 0)),
            pl.BlockSpec((ys, 2 * count), lambda i: (i, 0)),
            pl.BlockSpec((ys, 2 * count), lambda i: (i, 0)),
        ],
        out_shape=[
            jax.ShapeDtypeStruct((3, y_local, z_local, points), jnp.bfloat16),
            jax.ShapeDtypeStruct((y_local, 2 * count), jnp.float32),
            jax.ShapeDtypeStruct((y_local, 2 * count), jnp.float32),
        ],
        scratch_shapes=[pltpu.VMEM((3, ys * z_local, rows * kx_pad), jnp.bfloat16)] * 2,
        compiler_params=pltpu.CompilerParams(vmem_limit_bytes=VMEM_LIMIT),
        name="along_x",
    )(
        *arrived,
        x_table(kx, points, rows),
        phase_x,
        weights,
        jnp.concatenate([cos_z, cos_z], 1),
        jnp.concatenate([sin_z, sin_z], 1),
    )
    real_part = by_cos[:, :count] + by_sin[:, count:]
    imag_part = by_cos[:, count:] - by_sin[:, :count]
    cos_y, sin_y = jnp.cos(angle_y), jnp.sin(angle_y)
    terms = jnp.stack(
        [
            jnp.sum(real_part * cos_y + imag_part * sin_y, 0),
            jnp.sum(imag_part * cos_y - real_part * sin_y, 0),
        ],
        0,
    )
    spectrum = terms.reshape(2, freqs, dirs) * (wavenumbers * wavenumbers)[None, :, None]
    spectrum = jnp.transpose(spectrum / points**1.5, (2, 0, 1))
    total = lax.psum(spectrum, ("row", "col"))
    owned = dirs // cols
    far_field = lax.dynamic_slice_in_dim(total, lax.axis_index("col") * owned, owned, 0)
    return (velocity, far_field)


def velocity_points(modes):
    return 1 << (modes - 1).bit_length()


def solution(mesh):
    return jax.shard_map(
        functools.partial(body, mesh.shape["row"], mesh.shape["col"]),
        mesh=mesh,
        in_specs=(P(None, "row", "col", None), P(), P(), P()),
        out_specs=(P(None, "row", "col", None), P("col", None, None)),
        check_vma=False,
    )
```
